32 devices in a mesh: dp: 8 (over z, y), expert: 4 (over x, core).
Axes of the slice: x: 2, y: 2, z: 4, core: 2. Of those that a mesh axis runs over, the one named last changes fastest.
Arguments:
- grad_parts: bfloat16 [8, 2048, 6144], P('dp', 'expert')
- bucket_order: int32 [256], replicated, may hold values from 0 to 255, each once
- master: float32 [4, 8, 64, 6144], P('expert', 'dp'), may hold values from -6 to 6
- first_moment: float32 [4, 8, 64, 6144], P('expert', 'dp'), may hold values from -0.6 to 0.6
- second_moment: float32 [4, 8, 64, 6144], P('expert', 'dp'), may hold values from 0.01 to 1
- step_count: int32 [4, 8, 64], P('expert', 'dp'), may hold values from 1 to 8
- max_rms: float32 [1], replicated, may hold values from 0.3 to 1
Outputs:
- new_master: float32 [4, 8, 64, 6144], P('expert', 'dp')
- new_first: float32 [4, 8, 64, 6144], P('expert', 'dp')
- new_second: float32 [4, 8, 64, 6144], P('expert', 'dp')
- new_params: bfloat16 [2048, 6144], P('expert')
The draws below stay inside these ranges and needn't reach their ends.
Inputs may be any that keep to these rules, and one draw needn't show every extreme that they name: bucket_order is a permutation of the 256 buckets.
All inputs are finite; a program needn't handle non-finite values.
Results may differ from the reference program's by a relative error of at most 0.0085.
Values may be sent and summed in bfloat16 or wider, within the bound.
No kernel may reach another device: no remote copies, remote signals or barrier semaphores. Data moves between devices by JAX's collectives and lax.ppermute only.
A program may use at most 128 MiB of HBM per device.

```python
import math
import jax
import jax.numpy as jnp
from jax import lax

D = 6144
BROWS = 2
NBK = 256
ROWS = 2048
OWN = 64
N_DP = 8
N_EXPERT = 4


def draw_grad_parts(key, part):
    key_base = jax.random.fold_in(key, 11)
    key_rows = jax.random.fold_in(key, 12)
    base = jax.random.normal(key_base, (N_DP, ROWS, D), jnp.float32)
    ramp = jnp.exp(jnp.log(3.0) * jnp.arange(N_DP, dtype=jnp.float32) / max(N_DP - 1, 1)).reshape(N_DP, 1, 1)
    row_scale = jnp.exp(jax.random.uniform(key_rows, (1, ROWS, 1), jnp.float32) * jnp.log(10.0))
    return (base * row_scale * ramp).astype(jnp.bfloat16)


def set_ends(array, stream_key, smallest, top_value):
    place = [jax.random.randint(jax.random.fold_in(stream_key, axis), (), 0, length) for axis, length in enumerate(array.shape)]
    longest = array.shape.index(max(array.shape))
    neighbour = place[:longest] + [(place[longest] + 1) % array.shape[longest]] + place[longest + 1:]
    return array.at[tuple(place)].set(smallest).at[tuple(neighbour)].set(top_value)


def block_scale(key, dims, cuts, smallest, high):
    gain = 1.0
    for dim, shards_of in cuts:
        draws = jax.random.uniform(jax.random.fold_in(jax.random.fold_in(key, 6), dim), (shards_of,), jnp.float32, smallest / len(cuts), high / len(cuts))
        gain = gain * jnp.repeat(jnp.exp(draws), dims[dim] // shards_of).reshape((-1,) + (1,) * (len(dims) - 1 - dim))
    return gain


def noise(key, dims, width, bound, split=(), held_as=jnp.bfloat16):
    level = block_scale(key, dims, split, -0.22, 0.18) if split else 1.0
    result = jax.random.normal(key, dims, jnp.float32) * width * level
    return jnp.minimum(jnp.maximum(result, -bound), bound).astype(held_as)


def setup_inputs(seed: int = 0) -> dict:
    streams_of = jax.random.split(jax.random.key(seed), 8)
    return {
        "grad_parts": draw_grad_parts(jax.random.fold_in(streams_of[7], 71), 0),
        "bucket_order": jax.random.permutation(streams_of[1], NBK).astype(jnp.int32),
        "master": noise(streams_of[2], (N_EXPERT, N_DP, OWN, D), 1.0, 6.0, ((0, 4), (1, 8)), jnp.float32),
        "first_moment": noise(streams_of[3], (N_EXPERT, N_DP, OWN, D), 0.1, 0.6, ((0, 4), (1, 8)), jnp.float32),
        "second_moment": jnp.clip(jnp.exp(math.log(1.0) - 4.6051702 * jax.random.uniform(streams_of[4], (N_EXPERT, N_DP, OWN, D), jnp.float32) ** block_scale(streams_of[4], (N_EXPERT, N_DP, OWN, D), ((0, 4), (1, 8)), -0.2, 0.2)), 0.01, 1.0),
        "step_count": set_ends(jax.random.randint(streams_of[5], (N_EXPERT, N_DP, OWN), 1, 9), jax.random.fold_in(streams_of[5], 1), 1, 8).astype(jnp.int32),
        "max_rms": jnp.clip(jax.random.uniform(streams_of[6], (1,), jnp.float32, 0.3, 1.0), 0.3, 1.0),
    }


def reference(grad_parts, bucket_order, master, first_moment, second_moment, step_count, max_rms):

    def accumulate(index, running):
        piece = lax.dynamic_index_in_dim(grad_parts, index, 0, keepdims=False)
        return running + piece.astype(jnp.float32)
    grad_total = lax.fori_loop(0, N_DP, accumulate, jnp.zeros((ROWS, D), jnp.float32))
    square_sum = jnp.sum(grad_total * grad_total)
    entries = float(ROWS * D)
    clip_factor = jnp.minimum(1.0, max_rms[0] / jnp.sqrt(square_sum / entries + 1e-06))
    blocks = grad_total.reshape(N_EXPERT, NBK, BROWS, D)[:, bucket_order]
    slotted = blocks.reshape(N_EXPERT, N_DP, OWN, D)
    clipped = clip_factor * slotted
    new_first = 0.9 * first_moment + 0.1 * clipped
    new_second = 0.95 * second_moment + 0.05 * clipped * clipped
    step_float = step_count.astype(jnp.float32)[..., None]
    first_fix = 1.0 - jnp.power(jnp.float32(0.9), step_float)
    second_fix = 1.0 - jnp.power(jnp.float32(0.95), step_float)
    ratio = new_first / first_fix / (jnp.sqrt(new_second / second_fix) + 1e-08)
    new_master = master - 0.1 * (ratio + 0.1 * master)
    rounded = new_master.astype(jnp.bfloat16).reshape(N_EXPERT, NBK, BROWS, D)
    placed = jnp.zeros_like(rounded).at[:, bucket_order].set(rounded)
    return (new_master, new_first, new_second, placed.reshape(ROWS, D))
```

```python
import functools

import jax
import jax.numpy as jnp
from jax import lax
from jax.experimental import pallas as pl
from jax.experimental.pallas import tpu as pltpu
from jax.sharding import PartitionSpec as P

LANES = 128


def tile_of(width, limit=768):
    return max(t for t in range(LANES, limit + 1, LANES) if width % t == 0)


def column_parts(width):
    tiles = width // LANES
    cut = (tiles * 3 // 4) * LANES
    return [(0, cut), (cut, width)]


def bit_orders(bits):
    plain = list(range(bits))
    swapped = [1, 0] + plain[2:] if bits > 1 else plain
    return [plain, swapped]


def via(piece, order):
    return next(b for b in order if piece >> b & 1)


def exchange(x, bit, n):
    return lax.ppermute(x, "dp", [(i, i ^ (1 << bit)) for i in range(n)])


def slot_kernel(n, place_ref, grad_ref, *outs):
    rows = outs[0].shape[0]
    sorted_rows = jnp.dot(place_ref[...], grad_ref[0], preferred_element_type=jnp.float32)
    for piece in range(n):
        outs[piece][...] = sorted_rows[piece * rows:(piece + 1) * rows].astype(jnp.bfloat16)


def to_slots(place, grad, start, stop, n):
    rows = grad.shape[1]
    width = stop - start
    tile = tile_of(width)
    while start % tile:
        tile -= LANES
        while width % tile:
            tile -= LANES
    first = start // tile
    piece = jax.ShapeDtypeStruct((rows // n, width), jnp.bfloat16)
    return pl.pallas_call(
        functools.partial(slot_kernel, n),
        grid=(width // tile,),
        in_specs=[
            pl.BlockSpec((rows, rows), lambda i: (0, 0)),
            pl.BlockSpec((1, rows, tile), lambda i: (0, 0, i + first)),
        ],
        out_specs=[pl.BlockSpec((rows // n, tile), lambda i: (0, i))] * n,
        out_shape=[piece] * n,
        cost_estimate=pl.CostEstimate(
            flops=2 * rows * rows * width, bytes_accessed=4 * rows * width, transcendentals=0
        ),
        name="to_slots",
    )(place, grad)


def row_kernel(n, place_ref, *refs):
    pieces, out_ref = refs[:n], refs[-1]
    stacked = jnp.concatenate([p[...] for p in pieces], axis=0)
    out_ref[...] = jnp.dot(
        place_ref[...], stacked, preferred_element_type=jnp.float32
    ).astype(jnp.bfloat16)


def to_rows(place_t, pieces, start, total, earlier):
    n = len(pieces)
    rows = place_t.shape[0]
    width = pieces[0].shape[1]
    tile = tile_of(width)
    while start % tile:
        tile -= LANES
        while width % tile:
            tile -= LANES
    first = start // tile
    more = [] if earlier is None else [earlier]
    return pl.pallas_call(
        functools.partial(row_kernel, n),
        grid=(width // tile,),
        in_specs=[pl.BlockSpec((rows, rows), lambda i: (0, 0))]
        + [pl.BlockSpec((rows // n, tile), lambda i: (0, i))] * n
        + [pl.BlockSpec(memory_space=pl.ANY)] * len(more),
        out_specs=pl.BlockSpec((rows, tile), lambda i: (0, i + first)),
        out_shape=jax.ShapeDtypeStruct((rows, total), jnp.bfloat16),
        input_output_aliases={n + 1: 0} if more else {},
        cost_estimate=pl.CostEstimate(
            flops=2 * rows * rows * width, bytes_accessed=4 * rows * width, transcendentals=0
        ),
        name="to_rows",
    )(place_t, *pieces, *more)


def reduce_pieces(parts, order, n):
    f32 = jnp.float32
    terms = [[p] for p in parts]
    todo = sorted(range(1, n), key=lambda j: (order.index(via(j, order)), [-(j >> b & 1) for b in reversed(order)]))
    for j in todo:
        b = via(j, order)
        total = sum((t.astype(f32) for t in terms[j][1:]), terms[j][0].astype(f32))
        terms[j ^ (1 << b)].append(exchange(total.astype(jnp.bfloat16), b, n))
    return sum((t.astype(f32) for t in terms[0][1:]), terms[0][0].astype(f32))


def gather_pieces(own, order, n):
    have = {0: own}
    todo = sorted(range(1, n), key=lambda j: bin(j).count("1"))
    for j in todo:
        b = via(j, order)
        have[j] = exchange(have[j ^ (1 << b)], b, n)
    return [have[j] for j in range(n)]


def shards(grad_parts, bucket_order, master, first_moment, second_moment, step_count, max_rms):
    f32 = jnp.float32
    n = lax.axis_size("dp")
    groups = lax.axis_size("expert")
    me = lax.axis_index("dp")
    bits = n.bit_length() - 1
    _, rows_dev, row_width = grad_parts.shape
    bucket_count = bucket_order.shape[0]
    bucket_rows = rows_dev // bucket_count

    owners = me ^ jnp.arange(n, dtype=jnp.int32)
    pick = owners[:, None] == jnp.arange(n, dtype=jnp.int32)[None, :]
    order = bucket_order.reshape(n, bucket_count // n)
    relative = jnp.sum(jnp.where(pick[:, :, None], order[None], 0), axis=1).reshape(-1)
    target = (relative[:, None] * bucket_rows + jnp.arange(bucket_rows, dtype=jnp.int32)).reshape(-1)
    rows = jnp.arange(rows_dev, dtype=jnp.int32)
    place = (target[:, None] == rows[None, :]).astype(jnp.bfloat16)
    place_t = (rows[:, None] == target[None, :]).astype(jnp.bfloat16)

    parts = column_parts(row_width)
    orders = bit_orders(bits)
    owned, squares = [], []
    for (start, stop), bit_order in zip(parts, orders):
        pieces = to_slots(place, grad_parts, start, stop, n)
        total = reduce_pieces(pieces, bit_order, n)
        owned.append(total)
        squares.append(jnp.sum(total * total))
    local_square = sum(squares[1:], squares[0])
    copies = jnp.broadcast_to(local_square, (n * groups, 8, LANES))
    square_sum = jnp.sum(lax.all_to_all(copies, ("dp", "expert"), 0, 0)[:, 0, 0])
    entries = float(rows_dev * row_width * groups)
    clip_factor = jnp.minimum(1.0, max_rms[0] / jnp.sqrt(square_sum / entries + 1e-06))

    step_float = step_count[0, 0].astype(f32)[:, None]
    first_fix = 1.0 - jnp.power(f32(0.9), step_float)
    second_fix = 1.0 - jnp.power(f32(0.95), step_float)

    def adam(total, old_master, old_first, old_second):
        clipped = clip_factor * total
        new_first = 0.9 * old_first + 0.1 * clipped
        new_second = 0.95 * old_second + 0.05 * clipped * clipped
        ratio = new_first / first_fix / (jnp.sqrt(new_second / second_fix) + 1e-08)
        new_master = old_master - 0.1 * (ratio + 0.1 * old_master)
        return new_master, new_first, new_second

    placed = None
    results = []
    for (start, stop), bit_order, total in zip(parts, orders, owned):
        new_master, new_first, new_second = adam(
            total, master[0, 0, :, start:stop], first_moment[0, 0, :, start:stop], second_moment[0, 0, :, start:stop]
        )
        results.append((new_master, new_first, new_second))
        have = gather_pieces(new_master.astype(jnp.bfloat16), bit_order, n)
        placed = to_rows(place_t, have, start, row_width, placed)
    new_master, new_first, new_second = (jnp.concatenate(r, axis=1) for r in zip(*results))
    return new_master[None, None], new_first[None, None], new_second[None, None], placed


def solution(mesh):
    return jax.shard_map(
        shards,
        mesh=mesh,
        in_specs=(
            P("dp", "expert", None),
            P(),
            P("expert", "dp", None, None),
            P("expert", "dp", None, None),
            P("expert", "dp", None, None),
            P("expert", "dp", None),
            P(),
        ),
        out_specs=(
            P("expert", "dp", None, None),
            P("expert", "dp", None, None),
            P("expert", "dp", None, None),
            P("expert", None),
        ),
        check_vma=False,
    )
```

```python
import functools

import jax
import jax.numpy as jnp
from jax import lax
from jax.experimental import pallas as pl
from jax.experimental.pallas import tpu as pltpu
from jax.sharding import PartitionSpec as P


LANES = 128


def tile_of(width, limit=768):
    return max(t for t in range(LANES, limit + 1, LANES) if width % t == 0)


def column_parts(width):
    tiles = width // LANES
    ends = [0, tiles // 2 * LANES, tiles * 3 // 4 * LANES, width]
    return list(zip(ends[:-1], ends[1:]))


def bit_orders(bits):
    plain = list(range(bits))
    swapped = [1, 0] + plain[2:] if bits > 1 else plain
    return [plain, plain, swapped]


def via(piece, order):
    return next(b for b in order if piece >> b & 1)


def exchange(x, bit, n):
    return lax.ppermute(x, "dp", [(i, i ^ (1 << bit)) for i in range(n)])


def slot_kernel(me_ref, target_ref, grad_ref, *refs):
    outs, place_ref = refs[:-1], refs[-1]
    size = outs[0].shape[0]

    @pl.when(pl.program_id(0) == 0)
    def _():
        spots = lax.broadcasted_iota(jnp.int32, (size, place_ref.shape[1]), 1)
        for j in range(len(outs)):
            at = pl.multiple_of((me_ref[0] ^ j) * size, size)
            hit = target_ref[pl.ds(at, size), :] == spots
            place_ref[j * size:(j + 1) * size, :] = jnp.where(hit, 1.0, 0.0).astype(jnp.bfloat16)

    sorted_rows = jnp.dot(place_ref[...], grad_ref[0], preferred_element_type=jnp.float32)
    for j, out in enumerate(outs):
        out[...] = sorted_rows[j * size:(j + 1) * size].astype(jnp.bfloat16)


def whole_tile(start, width):
    tile = tile_of(width)
    while start % tile or width % tile:
        tile -= LANES
    return tile


def to_slots(me, targets, grad, start, stop, n):
    rows = grad.shape[1]
    width = stop - start
    tile = whole_tile(start, width)
    first = start // tile
    return pl.pallas_call(
        slot_kernel,
        grid=(width // tile,),
        in_specs=[
            pl.BlockSpec(memory_space=pltpu.SMEM),
            pl.BlockSpec((rows, 1), lambda i: (0, 0)),
            pl.BlockSpec((1, rows, tile), lambda i: (0, 0, i + first)),
        ],
        out_specs=[pl.BlockSpec((rows // n, tile), lambda i: (0, i))] * n,
        out_shape=[jax.ShapeDtypeStruct((rows // n, width), jnp.bfloat16)] * n,
        scratch_shapes=[pltpu.VMEM((rows, rows), jnp.bfloat16)],
        cost_estimate=pl.CostEstimate(
            flops=2 * rows * rows * width, bytes_accessed=4 * rows * width, transcendentals=0
        ),
        name="to_slots",
    )(me, targets, grad)


def row_kernel(n, target_ref, *refs):
    pieces, (out_ref, place_ref) = refs[:n], refs[-2:]

    @pl.when(pl.program_id(0) == 0)
    def _():
        spots = lax.broadcasted_iota(jnp.int32, place_ref.shape, 0)
        place_ref[...] = jnp.where(target_ref[...] == spots, 1.0, 0.0).astype(jnp.bfloat16)

    stacked = jnp.concatenate([p[...] for p in pieces], axis=0)
    out_ref[...] = jnp.dot(
        place_ref[...], stacked, preferred_element_type=jnp.float32
    ).astype(jnp.bfloat16)


def to_rows(target, pieces, start, total, earlier):
    n = len(pieces)
    rows = target.shape[1]
    width = pieces[0].shape[1]
    tile = whole_tile(start, width)
    first = start // tile
    more = [] if earlier is None else [earlier]
    return pl.pallas_call(
        functools.partial(row_kernel, n),
        grid=(width // tile,),
        in_specs=[pl.BlockSpec((1, rows), lambda i: (0, 0))]
        + [pl.BlockSpec((rows // n, tile), lambda i: (0, i))] * n
        + [pl.BlockSpec(memory_space=pl.ANY)] * len(more),
        out_specs=pl.BlockSpec((rows, tile), lambda i: (0, i + first)),
        out_shape=jax.ShapeDtypeStruct((rows, total), jnp.bfloat16),
        input_output_aliases={n + 1: 0} if more else {},
        scratch_shapes=[pltpu.VMEM((rows, rows), jnp.bfloat16)],
        cost_estimate=pl.CostEstimate(
            flops=2 * rows * rows * width, bytes_accessed=4 * rows * width, transcendentals=0
        ),
        name="to_rows",
    )(target, *pieces, *more)


REDUCE_8 = (
    "B7 B5 C7 C6",
    "A7 -C7 C5 -B7",
    "B6 A5 C3 C2",
    "-B5 -B6 B4 -A7",
    "A6 B3 -C5 -C6",
    "C4 A3 -A5 -A6",
    "A4 -C3 C1 -B3",
    "B2 B1 -A3 A2",
    "A1",
)
GATHER_8 = (
    "A1 A2 A4 C1",
    "B1 -A2 A3 -A4",
    "A6 A5 C4 B4",
    "-C1 C2 C3 B2",
    "-A6 A7 -C4 C5",
    "C6 -B2 B3 -B4",
    "B5 B6 -C5 C7",
    "-B6 B7",
)


def steps_of(text):
    return [(w.startswith("-"), "ABC".index(w[-2]), int(w[-1])) for part in text for w in part.split()]


def start_order(text, n, orders, leaves_first):
    if n == 8:
        return [(c, j) for done, c, j in steps_of(text) if not done]
    sign = -1 if leaves_first else 1
    return [
        (c, j)
        for c in range(len(orders))
        for j in sorted(range(1, n), key=lambda j: sign * bin(j).count("1"))
    ]


def add_up(terms):
    return sum((t.astype(jnp.float32) for t in terms[1:]), terms[0].astype(jnp.float32))


def reduce_pieces(parts, orders, n):
    terms = [{j: [p] for j, p in pieces.items()} for pieces in parts]
    for c, j in start_order(REDUCE_8, n, orders, True):
        b = via(j, orders[c])
        total = add_up(terms[c][j]).astype(jnp.bfloat16)
        terms[c][j ^ (1 << b)].append(exchange(total, b, n))
    return [add_up(t[0]) for t in terms]


def gather_pieces(owned, orders, n):
    have = [{0: x} for x in owned]
    for c, j in start_order(GATHER_8, n, orders, False):
        b = via(j, orders[c])
        have[c][j] = exchange(have[c][j ^ (1 << b)], b, n)
    return [[h[j] for j in range(n)] for h in have]


def shards(grad_parts, bucket_order, master, first_moment, second_moment, step_count, max_rms):
    f32 = jnp.float32
    n = lax.axis_size("dp")
    groups = lax.axis_size("expert")
    me = lax.axis_index("dp")
    bits = n.bit_length() - 1
    _, rows_dev, row_width = grad_parts.shape
    bucket_count = bucket_order.shape[0]
    bucket_rows = rows_dev // bucket_count

    cuts = column_parts(row_width)
    orders = bit_orders(bits)
    spread = jnp.arange(bucket_rows, dtype=jnp.int32)
    targets = (bucket_order[:, None] * bucket_rows + spread).reshape(rows_dev, 1)
    mine = me.astype(jnp.int32).reshape(1)
    raw = [{} for _ in cuts]
    for c in (1, 2, 0):
        raw[c] = dict(enumerate(to_slots(mine, targets, grad_parts, *cuts[c], n)))

    owners = me ^ jnp.arange(n, dtype=jnp.int32)
    pick = owners[:, None] == jnp.arange(n, dtype=jnp.int32)[None, :]
    order = bucket_order.reshape(n, bucket_count // n)
    relative = jnp.sum(jnp.where(pick[:, :, None], order[None], 0), axis=1)
    by_row = (relative[:, :, None] * bucket_rows + spread).reshape(1, rows_dev)
    owned = reduce_pieces(raw, orders, n)
    squares = [jnp.sum(t * t) for t in owned]
    local_square = sum(squares[1:], squares[0])
    copies = jnp.broadcast_to(local_square, (n * groups, 8, LANES))
    square_sum = jnp.sum(lax.all_to_all(copies, ("dp", "expert"), 0, 0)[:, 0, 0])
    entries = float(rows_dev * row_width * groups)
    clip_factor = jnp.minimum(1.0, max_rms[0] / jnp.sqrt(square_sum / entries + 1e-06))

    step_float = step_count[0, 0].astype(f32)[:, None]
    first_fix = 1.0 - jnp.power(f32(0.9), step_float)
    second_fix = 1.0 - jnp.power(f32(0.95), step_float)

    def adam(clip, total, old_master, old_first, old_second):
        clipped = clip * total
        new_first = 0.9 * old_first + 0.1 * clipped
        new_second = 0.95 * old_second + 0.05 * clipped * clipped
        ratio = new_first / first_fix / (jnp.sqrt(new_second / second_fix) + 1e-08)
        new_master = old_master - 0.1 * (ratio + 0.1 * old_master)
        return new_master, new_first, new_second

    def state_of(c):
        return [x[0, 0, :, cuts[c][0]:cuts[c][1]] for x in (master, first_moment, second_moment)]

    fresh = [adam(clip_factor, t, *state_of(c))[0].astype(jnp.bfloat16) for c, t in enumerate(owned)]
    have = gather_pieces(fresh, orders, n)
    placed = None
    for c in (0, 2, 1):
        placed = to_rows(by_row, have[c], cuts[c][0], row_width, placed)
    later_clip, later_owned = lax.optimization_barrier((clip_factor, owned))
    results = [adam(later_clip, t, *state_of(c)) for c, t in enumerate(later_owned)]
    new_master, new_first, new_second = (jnp.concatenate(r, axis=1) for r in zip(*results))
    return new_master[None, None], new_first[None, None], new_second[None, None], placed


def solution(mesh):
    return jax.shard_map(
        shards,
        mesh=mesh,
        in_specs=(
            P("dp", "expert", None),
            P(),
            P("expert", "dp", None, None),
            P("expert", "dp", None, None),
            P("expert", "dp", None, None),
            P("expert", "dp", None),
            P(),
        ),
        out_specs=(
            P("expert", "dp", None, None),
            P("expert", "dp", None, None),
            P("expert", "dp", None, None),
            P("expert", None),
        ),
        check_vma=False,
    )
```

```python
import functools
import math

import jax
import jax.numpy as jnp
from jax import lax
from jax.experimental import pallas as pl
from jax.experimental.pallas import tpu as pltpu
from jax.sharding import PartitionSpec as P


LANES = 128
ROW_TILE = 512
VMEM_LIMIT = 24 << 20


def tile_of(width, limit=768):
    return max(t for t in range(LANES, limit + 1, LANES) if width % t == 0)


def column_parts(width):
    tiles = width // LANES
    ends = [0, tiles // 2 * LANES, tiles * 3 // 4 * LANES, width]
    return list(zip(ends[:-1], ends[1:]))


def bit_orders(bits):
    plain = list(range(bits))
    swapped = [1, 0] + plain[2:] if bits > 1 else plain
    return [plain, plain, swapped]


def via(piece, order):
    return next(b for b in order if piece >> b & 1)


def exchange(x, bit, n):
    return lax.ppermute(x, "dp", [(i, i ^ (1 << bit)) for i in range(n)])


def slot_kernel(me_ref, target_ref, grad_ref, *refs):
    outs, place_ref = refs[:-1], refs[-1]
    size = outs[0].shape[0]

    @pl.when(pl.program_id(0) == 0)
    def _():
        spots = lax.broadcasted_iota(jnp.int32, (size, place_ref.shape[1]), 1)
        for j in range(len(outs)):
            at = pl.multiple_of((me_ref[0] ^ j) * size, size)
            hit = target_ref[pl.ds(at, size), :] == spots
            place_ref[j * size:(j + 1) * size, :] = jnp.where(hit, 1.0, 0.0).astype(jnp.bfloat16)

    sorted_rows = jnp.dot(place_ref[...], grad_ref[0], preferred_element_type=jnp.float32)
    for j, out in enumerate(outs):
        out[...] = sorted_rows[j * size:(j + 1) * size].astype(jnp.bfloat16)


def whole_tile(start, width):
    tile = tile_of(width)
    while start % tile or width % tile:
        tile -= LANES
    return tile


def to_slots(me, targets, grad, start, stop, n):
    rows = grad.shape[1]
    width = stop - start
    tile = whole_tile(start, width)
    first = start // tile
    return pl.pallas_call(
        slot_kernel,
        grid=(width // tile,),
        in_specs=[
            pl.BlockSpec(memory_space=pltpu.SMEM),
            pl.BlockSpec((rows, 1), lambda i: (0, 0)),
            pl.BlockSpec((1, rows, tile), lambda i: (0, 0, i + first)),
        ],
        out_specs=[pl.BlockSpec((rows // n, tile), lambda i: (0, i))] * n,
        out_shape=[jax.ShapeDtypeStruct((rows // n, width), jnp.bfloat16)] * n,
        scratch_shapes=[pltpu.VMEM((rows, rows), jnp.bfloat16)],
        compiler_params=pltpu.CompilerParams(vmem_limit_bytes=VMEM_LIMIT),
        cost_estimate=pl.CostEstimate(
            flops=2 * rows * rows * width, bytes_accessed=4 * rows * width, transcendentals=0
        ),
        name="to_slots",
    )(me, targets, grad)


def row_kernel(n, starts, widths, tile, me_ref, target_ref, *refs):
    pieces, (out_ref, place_ref, sorted_ref, done_ref, sems) = refs[:n * len(starts)], refs[-5:]
    size = pieces[0].shape[0]
    spots = lax.broadcasted_iota(jnp.int32, place_ref.shape, 0)
    place_ref[...] = jnp.where(target_ref[...] == spots, 1.0, 0.0).astype(jnp.bfloat16)
    copies = []
    for k, (start, width) in enumerate(zip(starts, widths)):
        for t in range(0, width, tile):
            spot = len(copies)
            for j, piece in enumerate(pieces[k * n:(k + 1) * n]):
                at = pl.multiple_of((me_ref[0] ^ j) * size, size)
                sorted_ref[spot, pl.ds(at, size), :] = piece[:, t:t + tile]
            done_ref[spot] = jnp.dot(
                place_ref[...], sorted_ref[spot], preferred_element_type=jnp.float32
            ).astype(jnp.bfloat16)
            copy = pltpu.make_async_copy(
                done_ref.at[spot], out_ref.at[:, pl.ds(start + t, tile)], sems.at[spot]
            )
            copy.start()
            copies.append(copy)
    for copy in copies:
        copy.wait()


def to_rows(me, target, chunks, starts, total, earlier):
    n = len(chunks[0])
    rows = target.shape[1]
    widths = [c[0].shape[1] for c in chunks]
    tile = tile_of(math.gcd(*widths), ROW_TILE)
    tiles = sum(widths) // tile
    inside = pl.BlockSpec(memory_space=pltpu.VMEM)
    more = [] if earlier is None else [earlier]
    pieces = [p for c in chunks for p in c]
    return pl.pallas_call(
        functools.partial(row_kernel, n, starts, widths, tile),
        in_specs=[pl.BlockSpec(memory_space=pltpu.SMEM)]
        + [inside] * (1 + len(pieces))
        + [pl.BlockSpec(memory_space=pl.ANY)] * len(more),
        out_specs=pl.BlockSpec(memory_space=pl.ANY),
        out_shape=jax.ShapeDtypeStruct((rows, total), jnp.bfloat16),
        input_output_aliases={len(pieces) + 2: 0} if more else {},
        scratch_shapes=[
            pltpu.VMEM((rows, rows), jnp.bfloat16),
            pltpu.VMEM((tiles, rows, tile), jnp.bfloat16),
            pltpu.VMEM((tiles, rows, tile), jnp.bfloat16),
            pltpu.SemaphoreType.DMA((tiles,)),
        ],
        compiler_params=pltpu.CompilerParams(vmem_limit_bytes=VMEM_LIMIT),
        cost_estimate=pl.CostEstimate(
            flops=2 * rows * rows * sum(widths), bytes_accessed=4 * rows * sum(widths), transcendentals=0
        ),
        name="to_rows",
    )(me, target, *pieces, *more)


REDUCE_8 = (
    "B7 B5 C7 C6",
    "A7 -C7 C5 -B7",
    "B6 A5 -B5 -B6",
    "B4 -A7 A6 C3",
    "A3 -C5 -C6 C4",
    "C2 B3 B1 -A5",
    "-A6 A4 A1 -A3",
    "A2 -C3 C1 -B3",
    "B2",
)
GATHER_8 = (
    "A1 A2 A4 C1",
    "B1 -A2 A3 -A4",
    "A6 A5 C4 B2",
    "-C4 C5 -A6 A7",
    "B4 C2 -C1 C3",
    "-B2 B3 -B4 B6",
    "B5 C6 -C5 C7",
    "-B6 B7",
)


def steps_of(text):
    return [(w.startswith("-"), "ABC".index(w[-2]), int(w[-1])) for part in text for w in part.split()]


def start_order(text, n, orders, leaves_first):
    if n == 8:
        return [(c, j) for done, c, j in steps_of(text) if not done]
    sign = -1 if leaves_first else 1
    return [
        (c, j)
        for c in range(len(orders))
        for j in sorted(range(1, n), key=lambda j: sign * bin(j).count("1"))
    ]


def add_up(terms):
    return sum((t.astype(jnp.float32) for t in terms[1:]), terms[0].astype(jnp.float32))


def reduce_pieces(parts, orders, n):
    terms = [{j: [p] for j, p in pieces.items()} for pieces in parts]
    for c, j in start_order(REDUCE_8, n, orders, True):
        b = via(j, orders[c])
        total = add_up(terms[c][j]).astype(jnp.bfloat16)
        terms[c][j ^ (1 << b)].append(exchange(total, b, n))
    return [t[0] for t in terms]


def gather_pieces(owned, orders, n):
    have = [{0: x} for x in owned]
    for c, j in start_order(GATHER_8, n, orders, False):
        b = via(j, orders[c])
        have[c][j] = exchange(have[c][j ^ (1 << b)], b, n)
    return [[h[j] for j in range(n)] for h in have]


def fold(x):
    rows, width = x.shape
    return sum(
        x[r:r + 8, t:t + LANES] for r in range(0, rows, 8) for t in range(0, width, LANES)
    )


def total_kernel(count, *refs):
    terms, others = refs[:count], refs[count:-2]
    total_ref, square_ref = refs[-2:]
    width = total_ref.shape[1]
    tile = tile_of(width, 512)
    acc = sum((o[...] for o in others[1:]), others[0][...]) if others else jnp.zeros((8, LANES), jnp.float32)
    for t in range(0, width, tile):
        total = terms[0][:, t:t + tile].astype(jnp.float32)
        for x in terms[1:]:
            total += x[:, t:t + tile].astype(jnp.float32)
        total_ref[:, t:t + tile] = total
        acc += fold(total * total)
    square_ref[...] = acc


def owned_total(terms, others):
    rows, width = terms[0].shape
    square = jax.ShapeDtypeStruct((8, LANES), jnp.float32)
    inside = pl.BlockSpec(memory_space=pltpu.VMEM)
    return pl.pallas_call(
        functools.partial(total_kernel, len(terms)),
        in_specs=[inside] * (len(terms) + len(others)),
        out_specs=[inside] * 2,
        out_shape=[jax.ShapeDtypeStruct((rows, width), jnp.float32), square],
        compiler_params=pltpu.CompilerParams(vmem_limit_bytes=VMEM_LIMIT),
        cost_estimate=pl.CostEstimate(
            flops=8 * rows * width, bytes_accessed=12 * rows * width, transcendentals=0
        ),
        name="owned_total",
    )(*terms, *others)


def pair_kernel(mine_ref, other_ref, out_ref):
    out_ref[...] = mine_ref[...] + other_ref[...]


def sum_over_mesh(x, axes):
    inside = pl.BlockSpec(memory_space=pltpu.VMEM)
    for axis, size in axes:
        for b in range(size.bit_length() - 1):
            other = lax.ppermute(x, axis, [(i, i ^ (1 << b)) for i in range(size)])
            x = pl.pallas_call(
                pair_kernel,
                in_specs=[inside] * 2,
                out_specs=inside,
                out_shape=jax.ShapeDtypeStruct(x.shape, x.dtype),
                compiler_params=pltpu.CompilerParams(vmem_limit_bytes=VMEM_LIMIT),
                name="pair_sum",
            )(x, other)
    return x


def column(row):
    size = row.shape[1]
    diagonal = lax.broadcasted_iota(jnp.int32, (size, size), 0) == lax.broadcasted_iota(jnp.int32, (size, size), 1)
    return jnp.sum(jnp.where(diagonal, row, 0.0), axis=1, keepdims=True)


def adam_factors(entries, squares_ref, rms_ref, steps_ref):
    square_sum = jnp.sum(jnp.sum(squares_ref[...], axis=0, keepdims=True), axis=1, keepdims=True)
    clip = jnp.minimum(1.0, rms_ref[0] / jnp.sqrt(square_sum / entries + 1e-06))
    steps = column(steps_ref[0].astype(jnp.float32))
    return clip, 1.0 - jnp.exp(steps * math.log(0.9)), 1.0 - jnp.exp(steps * math.log(0.95))


def adam(factors, total, master, first, second):
    clip, first_fix, second_fix = factors
    clipped = clip * total
    new_first = 0.9 * first + 0.1 * clipped
    new_second = 0.95 * second + 0.05 * clipped * clipped
    ratio = new_first / first_fix / (jnp.sqrt(new_second / second_fix) + 1e-08)
    return master - 0.1 * (ratio + 0.1 * master), new_first, new_second


def fresh_kernel(entries, start, squares_ref, rms_ref, steps_ref, total_ref, m_ref, f_ref, s_ref, out_ref):
    width = out_ref.shape[1]
    tile = tile_of(width, 512)
    factors = adam_factors(entries, squares_ref, rms_ref, steps_ref)
    for t in range(0, width, tile):
        state = [x[0, 0, :, start + t:start + t + tile] for x in (m_ref, f_ref, s_ref)]
        out_ref[:, t:t + tile] = adam(factors, total_ref[:, t:t + tile], *state)[0].astype(jnp.bfloat16)


def small_specs():
    inside = pl.BlockSpec(memory_space=pltpu.VMEM)
    return [inside, pl.BlockSpec(memory_space=pltpu.SMEM), inside]


def fresh_rows(entries, small, total, state, start):
    rows, width = total.shape
    inside = pl.BlockSpec(memory_space=pltpu.VMEM)
    return pl.pallas_call(
        functools.partial(fresh_kernel, entries, start),
        in_specs=small_specs() + [inside] * 4,
        out_specs=inside,
        out_shape=jax.ShapeDtypeStruct((rows, width), jnp.bfloat16),
        compiler_params=pltpu.CompilerParams(vmem_limit_bytes=VMEM_LIMIT),
        cost_estimate=pl.CostEstimate(
            flops=20 * rows * width, bytes_accessed=18 * rows * width, transcendentals=0
        ),
        name="fresh_rows",
    )(*small, total, *state)


def state_kernel(entries, firsts, squares_ref, rms_ref, steps_ref, *refs):
    totals, (m_ref, f_ref, s_ref), outs = refs[:len(firsts)], refs[len(firsts):-3], refs[-3:]
    step = pl.program_id(0)
    total = totals[0][...]
    for begin, ref in zip(firsts[1:], totals[1:]):
        total = jnp.where(step >= begin, ref[...], total)
    factors = adam_factors(entries, squares_ref, rms_ref, steps_ref)
    results = adam(factors, total, m_ref[0, 0], f_ref[0, 0], s_ref[0, 0])
    for out, result in zip(outs, results):
        out[0, 0] = result


def new_state(entries, small, totals, state):
    rows = totals[0].shape[0]
    widths = [t.shape[1] for t in totals]
    tile = tile_of(math.gcd(*widths))
    blocks = [w // tile for w in widths]
    firsts = [sum(blocks[:k]) for k in range(len(blocks))]
    inside = lambda begin, count: lambda i: (0, jnp.clip(i - begin, 0, count - 1))
    wide = pl.BlockSpec((1, 1, rows, tile), lambda i: (0, 0, 0, i))
    return pl.pallas_call(
        functools.partial(state_kernel, entries, firsts),
        grid=(sum(blocks),),
        in_specs=small_specs()
        + [pl.BlockSpec((rows, tile), inside(b, k)) for b, k in zip(firsts, blocks)]
        + [wide] * 3,
        out_specs=[wide] * 3,
        out_shape=[jax.ShapeDtypeStruct(x.shape, jnp.float32) for x in state],
        compiler_params=pltpu.CompilerParams(vmem_limit_bytes=VMEM_LIMIT),
        cost_estimate=pl.CostEstimate(
            flops=20 * rows * sum(widths), bytes_accessed=28 * rows * sum(widths), transcendentals=0
        ),
        name="new_state",
    )(*small, *totals, *state)


def shards(grad_parts, bucket_order, master, first_moment, second_moment, step_count, max_rms):
    n = lax.axis_size("dp")
    groups = lax.axis_size("expert")
    me = lax.axis_index("dp")
    bits = n.bit_length() - 1
    _, rows_dev, row_width = grad_parts.shape
    bucket_count = bucket_order.shape[0]
    bucket_rows = rows_dev // bucket_count

    cuts = column_parts(row_width)
    orders = bit_orders(bits)
    spread = jnp.arange(bucket_rows, dtype=jnp.int32)
    targets = (bucket_order[:, None] * bucket_rows + spread).reshape(rows_dev, 1)
    mine = me.astype(jnp.int32).reshape(1)
    raw = [{} for _ in cuts]
    for c in (1, 2, 0):
        raw[c] = dict(enumerate(to_slots(mine, targets, grad_parts, *cuts[c], n)))

    by_row = (bucket_order[:, None] * bucket_rows + spread).reshape(1, rows_dev)
    terms = reduce_pieces(raw, orders, n)
    owned = [None] * len(cuts)
    owned[2], square_2 = owned_total(terms[2], [])
    owned[1], square_1 = owned_total(terms[1], [])
    owned[0], square_0 = owned_total(terms[0], [square_1, square_2])
    squares = sum_over_mesh(square_0, (("expert", groups), ("dp", n)))
    entries = float(rows_dev * row_width * groups)

    small = (squares, max_rms, step_count)
    state = (master, first_moment, second_moment)
    fresh = [None] * len(cuts)
    for c in (0, 2, 1):
        fresh[c] = fresh_rows(entries, small, owned[c], state, cuts[c][0])
    have = gather_pieces(fresh, orders, n)
    results = new_state(entries, small, owned, state)
    placed = None
    for group in ((0,), (1, 2)):
        starts = [cuts[c][0] for c in group]
        placed = to_rows(mine, by_row, [have[c] for c in group], starts, row_width, placed)
    return *results, placed


def solution(mesh):
    return jax.shard_map(
        shards,
        mesh=mesh,
        in_specs=(
            P("dp", "expert", None),
            P(),
            P("expert", "dp", None, None),
            P("expert", "dp", None, None),
            P("expert", "dp", None, None),
            P("expert", "dp", None),
            P(),
        ),
        out_specs=(
            P("expert", "dp", None, None),
            P("expert", "dp", None, None),
            P("expert", "dp", None, None),
            P("expert", None),
        ),
        check_vma=False,
    )
```
